32 devices in a mesh: gz: 16 (over z, y, core), gy: 2 (over x).
Axes of the slice: x: 2, y: 2, z: 4, core: 2. Of those that a mesh axis runs over, the one named last changes fastest.
Arguments:
- estimate: float32 [256, 64, 512], P('gz', 'gy'), may hold values from 0.5 to 2
- measured: float32 [4, 256, 64, 512], P(None, 'gz', 'gy'), may hold values from 0.25 to 4
- psf_z: float32 [4, 31], replicated, may hold values from 0.1 to 1
- psf_y: float32 [4, 15], replicated, may hold values from 0.1 to 1
- psf_x: float32 [4, 15], replicated, may hold values from 0.1 to 1
- extents: int32 [4, 3], replicated, may hold values from 9 to 31, as said below
- order: int32 [4], replicated, may hold values from 0 to 3, each once
Outputs:
- updated: float32 [256, 64, 512], P('gz', 'gy')
The draws below stay inside these ranges and needn't reach their ends.
Inputs may be any that keep to these rules, and one draw needn't show every extreme that they name: `extents`: every extent is odd; along z it lies in 9 to 31, along y and x in 9 to 15; in every draw some view has extent 31 along z and some view has extent 15 along y.
All inputs are finite; a program needn't handle non-finite values.
Results may differ from the reference program's by a relative error of at most 0.0001.
Values sent between devices are 32-bit elements; how exact they have to be, the bound alone decides.
A program may use at most 64 MiB of HBM per device.

```python
import math
import jax
import jax.numpy as jnp
from jax import lax

NX = 512
V = 4
KZ = 31
KL = 15
NZ = 256
NY = 64


def draw_extents(key, part):
    keys = jax.random.split(jax.random.fold_in(key, 7), 5)
    radius_z = jax.random.randint(keys[0], (V,), 4, 16)
    radius_y = jax.random.randint(keys[1], (V,), 4, 8)
    radius_x = jax.random.randint(keys[2], (V,), 4, 8)
    views = jnp.arange(V, dtype=jnp.int32)
    pick_z = jax.random.randint(keys[3], (), 0, V)
    pick_y = jax.random.randint(keys[4], (), 0, V)
    radius_z = jnp.where(views == pick_z, 15, radius_z)
    radius_y = jnp.where(views == pick_y, 7, radius_y)
    radii = jnp.stack([radius_z, radius_y, radius_x], axis=1)
    return (2 * radii + 1).astype(jnp.int32)


def block_scale(own_key, dims, pieces, least, top_value):
    def one(axis_at, parts):
        heights = jax.random.uniform(jax.random.fold_in(jax.random.fold_in(own_key, 6), axis_at), (parts,), jnp.float32, least / len(pieces), top_value / len(pieces))
        return jnp.repeat(jnp.exp(heights), dims[axis_at] // parts).reshape((-1,) + (1,) * (len(dims) - axis_at - 1))

    level = one(*pieces[0])
    for cut in pieces[1:]:
        level = level * one(*cut)
    return level


def setup_inputs(seed: int = 0) -> dict:
    streams_of = jax.random.split(jax.random.key(seed), 8)
    return {
        "estimate": jnp.clip(jnp.exp(math.log(2.0) - 1.3862944 * jax.random.uniform(streams_of[0], (NZ, NY, NX), jnp.float32) ** block_scale(streams_of[0], (NZ, NY, NX), ((0, 16), (1, 2)), -0.2, 0.2)), 0.5, 2.0),
        "measured": jnp.clip(jnp.exp(math.log(4.0) - 2.7725887 * jax.random.uniform(streams_of[1], (V, NZ, NY, NX), jnp.float32) ** block_scale(streams_of[1], (V, NZ, NY, NX), ((1, 16), (2, 2)), -0.2, 0.2)), 0.25, 4.0),
        "psf_z": jnp.clip(jnp.exp(jax.random.uniform(streams_of[2], (V, KZ), jnp.float32, math.log(0.1), math.log(1.0))), 0.1, 1.0),
        "psf_y": jnp.clip(jnp.exp(jax.random.uniform(streams_of[3], (V, KL), jnp.float32, math.log(0.1), math.log(1.0))), 0.1, 1.0),
        "psf_x": jnp.clip(jnp.exp(jax.random.uniform(streams_of[4], (V, KL), jnp.float32, math.log(0.1), math.log(1.0))), 0.1, 1.0),
        "extents": draw_extents(jax.random.fold_in(streams_of[7], 71), 0),
        "order": jax.random.permutation(streams_of[6], V).astype(jnp.int32),
    }


def line_taps(profile, reach_cells, tap_reach):
    offsets = jnp.arange(2 * tap_reach + 1, dtype=jnp.int32) - tap_reach
    kept = jnp.where(jnp.abs(offsets) <= reach_cells, profile, jnp.zeros_like(profile))
    return kept / jnp.sum(kept)


def pad_axis(field, along_axis, tap_reach):
    widths = [(0, 0), (0, 0), (0, 0)]
    widths[along_axis] = (tap_reach, tap_reach)
    return jnp.pad(field, widths)


def correlate_padded(padded, weights, along_axis, tap_reach, length, flipped):
    total = None
    for offset in range(2 * tap_reach + 1):
        start = 2 * tap_reach - offset if flipped else offset
        piece = lax.slice_in_dim(padded, start, start + length, axis=along_axis)
        term = weights[offset] * piece
        total = term if total is None else total + term
    return total


def blur(field, weights_z, weights_y, weights_x, flipped):
    result = correlate_padded(pad_axis(field, 0, 15), weights_z, 0, 15, field.shape[0], flipped)
    result = correlate_padded(pad_axis(result, 1, 7), weights_y, 1, 7, field.shape[1], flipped)
    result = correlate_padded(pad_axis(result, 2, 7), weights_x, 2, 7, field.shape[2], flipped)
    return result


def reference(estimate, measured, psf_z, psf_y, psf_x, extents, order):
    current = estimate
    for position in range(V):
        view = order[position]
        radii = (extents[view] - 1) // 2
        weights_z = line_taps(psf_z[view], radii[0], 15)
        weights_y = line_taps(psf_y[view], radii[1], 7)
        weights_x = line_taps(psf_x[view], radii[2], 7)
        blurred = blur(current, weights_z, weights_y, weights_x, False)
        ratio = measured[view] / blurred
        current = current * blur(ratio, weights_z, weights_y, weights_x, True)
    return current
```

```python
import functools
import jax
import jax.numpy as jnp
from jax import lax
from jax.experimental import pallas as pl
from jax.experimental.pallas import tpu as pltpu
from jax.sharding import PartitionSpec as P

MESH = pl.DeviceIdType.MESH
RZ = 15
RL = 7
LANES = 128


def with_halo(value, sides, width):
    for axis, dim in sides:
        size, length = (lax.axis_size(axis), value.shape[dim])
        up = [(i, (i + 1) % size) for i in range(size - 1)]
        down = [(j, i) for i, j in up]
        last = lax.slice_in_dim(value, length - width, length, axis=dim)
        initial = lax.slice_in_dim(value, 0, width, axis=dim)
        before = lax.ppermute(last, axis, up)
        after = lax.ppermute(initial, axis, down)
        value = jnp.concatenate([before, value, after], axis=dim)
    return value


def line_taps(profile, reach_cells, tap_reach):
    offsets = jnp.arange(2 * tap_reach + 1, dtype=jnp.int32) - tap_reach
    kept = jnp.where(jnp.abs(offsets) <= reach_cells, profile, jnp.zeros_like(profile))
    return kept / jnp.sum(kept)


def correlate_padded(padded, weights, along_axis, tap_reach, length, flipped):
    total = None
    for offset in range(2 * tap_reach + 1):
        start = 2 * tap_reach - offset if flipped else offset
        piece = lax.slice_in_dim(padded, start, start + length, axis=along_axis)
        term = weights[offset] * piece
        total = term if total is None else total + term
    return total


def blur(field, weights_z, weights_y, weights_x, flipped):
    padded = with_halo(field, (("gz", 0),), RZ)
    result = correlate_padded(padded, weights_z, 0, RZ, field.shape[0], flipped)
    widened = with_halo(result, (("gy", 1),), RL)
    result = correlate_padded(widened, weights_y, 1, RL, field.shape[1], flipped)
    result = jnp.pad(result, ((0, 0), (0, 0), (RL, RL)))
    return correlate_padded(result, weights_x, 2, RL, field.shape[2], flipped)


def general(estimate, measured, psf_z, psf_y, psf_x, extents, order):
    current = estimate
    for position in range(measured.shape[0]):
        view = order[position]
        radii = (extents[view] - 1) // 2
        weights_z = line_taps(psf_z[view], radii[0], RZ)
        weights_y = line_taps(psf_y[view], radii[1], RL)
        weights_x = line_taps(psf_x[view], radii[2], RL)
        recorded = lax.dynamic_index_in_dim(measured, view, 0, keepdims=False)
        blurred = blur(current, weights_z, weights_y, weights_x, False)
        ratio = recorded / blurred
        current = current * blur(ratio, weights_z, weights_y, weights_x, True)
    return current


def place():
    g = lax.axis_index("gz")
    w = lax.axis_index("gy")
    return g // 4, (g // 2) % 2, g % 2, w


def slab_of(a, w):
    return 2 * a + lax.rem(w + a, 2)


def group_peers():
    h, a, c, w = place()
    peers = []
    for k in range(1, 8):
        da, dc, dw = k // 4, (k // 2) % 2, k % 2
        device = (4 * h + 2 * lax.rem(a + da, 2) + lax.rem(c + dc, 2), lax.rem(w + dw, 2))
        peers.append(device)
    return peers


def taps_of(profile, view, radius, reach):
    kept = []
    for k in range(2 * reach + 1):
        value = jnp.full((8, LANES), profile[view, k], jnp.float32)
        kept.append(jnp.where(abs(k - reach) <= radius, value, jnp.zeros_like(value)))
    total = kept[0]
    for value in kept[1:]:
        total = total + value
    return [value / total for value in kept]


def band(taps, which):
    total = jnp.zeros(which.shape, jnp.float32)
    for k, tap in enumerate(taps):
        total = jnp.where(which == k, tap[0:1, :], total)
    return split(total)


def split(value):
    hi = value.astype(jnp.bfloat16)
    lo = (value - hi.astype(jnp.float32)).astype(jnp.bfloat16)
    return hi, lo


ROWS = 8
LAG = 3


def wavefront_kernel(chain, nz, ny, views, est, measured, psf_z, psf_y, psf_x, extents, order, out,
                     wz, wy, xm, xe, f, zh, zb, yb, pack, got, stage, chosen, moved,
                     zs, zr, xs, xr, es, er, bs, br, gs, gr, el, gl, fl):
    h, a, c, w = place()
    zi = 2 * h + c
    s = slab_of(a, w)
    planes = 2 * nz
    chunks = 2 * ny // ROWS
    own = ny // ROWS
    blurs = 2 * views
    last = blurs * chunks
    has_dn, has_up = zi > 0, zi < chain - 1
    has_l, has_r = s > 0, s < 3
    home = c == a
    away = c != a

    def z_dev(i):
        return (4 * (i // 2) + 2 * a + lax.rem(i, 2), w)

    def x_dev(i):
        b = i // 2
        return (4 * h + 2 * b + c, lax.rem(i + b, 2))

    up, dn = z_dev(lax.rem(zi + 1, chain)), z_dev(lax.rem(zi + chain - 1, chain))
    lf, rt = x_dev(lax.rem(s + 3, 4)), x_dev(lax.rem(s + 1, 4))
    far_there = jnp.where(c == 1, h < chain // 2 - 1, h > 0)
    far = z_dev(jnp.where(c == 1, lax.rem(zi + 1, chain), lax.rem(zi + chain - 1, chain)))

    barrier = pltpu.get_barrier_semaphore()
    for device in group_peers():
        pl.semaphore_signal(barrier, inc=1, device_id=device, device_id_type=MESH)

    @pl.when(far_there)
    def _():
        pl.semaphore_signal(barrier, inc=1, device_id=far, device_id_type=MESH)

    fetch = pltpu.make_async_copy(measured, stage, fl)
    fetch.start()
    pl.semaphore_wait(barrier, 7 + far_there.astype(jnp.int32))

    def remote(src, dst, send, recv, device):
        return pltpu.make_async_remote_copy(src_ref=src, dst_ref=dst, send_sem=send, recv_sem=recv,
                                            device_id=device, device_id_type=MESH)

    def rows8(r):
        return pl.ds(pl.multiple_of(ROWS * r, ROWS), ROWS)

    def outward(r, k):
        da, dw = k // 2, k % 2
        ta, tw = lax.rem(c + da, 2), lax.rem(w + dw, 2)
        x0 = pl.multiple_of(LANES * slab_of(ta, tw), LANES)
        return (slice(None), rows8(r), pl.ds(x0, LANES)), (own * w + r, pl.ds(nz * c, nz)), (4 * h + 2 * ta + a, tw)

    def est_copy(r, k):
        there, here, device = outward(r, k)
        return remote(est.at[there], f.at[(0,) + here], es.at[r, k], er.at[r, k], device)

    def est_local(r):
        there, here, _ = outward(r, 0)
        return pltpu.make_async_copy(est.at[there], f.at[(0,) + here], el.at[r])

    def bulk(p, r, k):
        there, here, device = outward(r, k)
        return remote(chosen.at[(p,) + there], moved.at[(p,) + here], bs.at[p, r, k], br.at[p, r, k], device)

    def back(j, tc):
        tw, r = j // own, lax.rem(j, own)
        k = 2 * lax.rem(tc + a, 2) + lax.rem(tw + w, 2)
        x0 = pl.multiple_of(LANES * s, LANES)
        src = f.at[0, j, pl.ds(nz * tc, nz)]
        dst = out.at[:, rows8(r), pl.ds(x0, LANES)]
        return (remote(src, dst, gs.at[r, k], gr.at[r, k], (4 * h + 2 * c + tc, tw)),
                pltpu.make_async_copy(src, dst, gl.at[r]), jnp.logical_and(home, k == 0))

    def z_copy(side, par, j):
        if side == 0:
            return remote(f.at[par, j, pl.ds(planes - RZ, RZ)], zh.at[0, par, j], zs.at[0, par, j], zr.at[0, par, j], up)
        return remote(f.at[par, j, pl.ds(0, RZ)], zh.at[1, par, j], zs.at[1, par, j], zr.at[1, par, j], dn)

    def x_copy(side, par, j):
        if side == 0:
            return remote(pack.at[1, par, j], got.at[0, par, j], xs.at[0, par, j], xr.at[0, par, j], rt)
        return remote(pack.at[0, par, j], got.at[1, par, j], xs.at[1, par, j], xr.at[1, par, j], lf)

    def guarded(cond, act):
        @pl.when(cond)
        def _():
            act()

    for r in range(own):
        for k in range(1, 4):
            est_copy(r, k).start()
        guarded(away, lambda: est_copy(r, 0).start())
        guarded(home, lambda: est_local(r).start())

    build_weights(views, psf_z, psf_y, psf_x, extents, order, wz, wy, xm, xe)

    zb[...] = jnp.zeros_like(zb)

    def clear(ref, side):
        def one(i, carry):
            ref[side, i // chunks, lax.rem(i, chunks)] = jnp.zeros(ref.shape[3:], jnp.float32)
            return carry

        lax.fori_loop(0, 2 * chunks, one, 0)

    guarded(jnp.logical_not(has_dn), lambda: clear(zh, 0))
    guarded(jnp.logical_not(has_up), lambda: clear(zh, 1))
    guarded(jnp.logical_not(has_l), lambda: clear(got, 0))
    guarded(jnp.logical_not(has_r), lambda: clear(got, 1))

    fetch.wait()
    for p in range(views):
        def pick(i, carry):
            chosen[p, i] = stage[order[p], i]
            return carry

        lax.fori_loop(0, nz, pick, 0)

    def keep():
        x0 = pl.multiple_of(LANES * slab_of(c, w), LANES)
        for p in range(views):
            for r in range(own):
                moved[p, own * w + r, pl.ds(nz * c, nz)] = chosen[p, :, r * ROWS:(r + 1) * ROWS, pl.ds(x0, LANES)]

    guarded(home, keep)

    def send_z(par, j):
        guarded(has_up, lambda: z_copy(0, par, j).start())
        guarded(has_dn, lambda: z_copy(1, par, j).start())

    def enter(i):
        guarded(home, lambda: est_local(i).wait())
        guarded(away, lambda: est_copy(i, 0).wait_recv())
        for k in range(1, 4):
            est_copy(i, k).wait_recv()
        send_z(0, i)
        send_z(0, i + own)

    lane = lax.broadcasted_iota(jnp.int32, (ROWS, LANES), 1)
    per = LANES // 8
    half = 16

    def z_stage(t):
        k = t // chunks
        j = t - k * chunks
        par = lax.rem(k, 2)
        guarded(has_dn, lambda: z_copy(0, par, j).wait_recv())
        guarded(has_up, lambda: z_copy(1, par, j).wait_recv())
        taps = [wz[k, i] for i in range(2 * RZ + 1)]
        ys = pl.ds(pl.multiple_of(ROWS * j + ROWS, ROWS), ROWS)
        for first in range(0, planes, half):
            acc = [None] * half
            for p in range(first, first + half + 2 * RZ):
                if p < RZ:
                    v = zh[0, par, j, p]
                elif p < RZ + planes:
                    v = f[par, j, p - RZ]
                else:
                    v = zh[1, par, j, p - RZ - planes]
                for o in range(half):
                    i = p - first - o
                    if 0 <= i <= 2 * RZ:
                        term = taps[i] * v
                        acc[o] = term if acc[o] is None else acc[o] + term
            for o in range(half):
                zb[first + o, ys, :] = acc[o]

    def y_stage(t):
        k = t // chunks
        j = t - k * chunks
        par = lax.rem(k, 2)

        def reuse():
            guarded(has_r, lambda: x_copy(0, par, j).wait_send())
            guarded(has_l, lambda: x_copy(1, par, j).wait_send())

        guarded(k >= 2, reuse)
        taps = [wy[k, i] for i in range(2 * RL + 1)]
        base = pl.multiple_of(ROWS * j, ROWS)
        for q in range(planes // per):
            packed_l = packed_r = None
            for i in range(per):
                p = q * per + i
                value = None
                for o in range(2 * RL + 1):
                    term = taps[o] * zb[p, pl.ds(base + (o + ROWS - RL), ROWS), :]
                    value = term if value is None else value + term
                yb[j, p] = value
                at = 8 * i
                left = value if at == 0 else pltpu.roll(value, at, 1)
                right = pltpu.roll(value, (at + 8) % LANES, 1) if at + 8 < LANES else value
                packed_l = left if packed_l is None else jnp.where(lane >= at, left, packed_l)
                packed_r = right if packed_r is None else jnp.where(lane >= at, right, packed_r)
            pack[0, par, j, q] = packed_l
            pack[1, par, j, q] = packed_r
        guarded(has_r, lambda: x_copy(0, par, j).start())
        guarded(has_l, lambda: x_copy(1, par, j).start())

    step = 8

    def x_stage(t):
        k = t // chunks
        j = t - k * chunks
        par = lax.rem(k, 2)
        even = par == 0
        p_view = k // 2
        nxt = lax.rem(k + 1, 2)
        guarded(has_l, lambda: x_copy(0, par, j).wait_recv())
        guarded(has_r, lambda: x_copy(1, par, j).wait_recv())

        def sent():
            guarded(has_up, lambda: z_copy(0, nxt, j).wait_send())
            guarded(has_dn, lambda: z_copy(1, nxt, j).wait_send())

        guarded(k >= 1, sent)

        def body(divide):
            if divide:
                dw = lax.rem(w + j // own, 2)
                r = lax.rem(j, own)
                for da in range(2):
                    if da == 0:
                        guarded(jnp.logical_or(away, dw > 0), lambda: bulk(p_view, r, dw).wait_recv())
                    else:
                        bulk(p_view, r, 2 + dw).wait_recv()
            for p in range(0, planes, step):
                edges = []
                for i in range(step):
                    q, n = divmod(p + i, per)
                    left, right = got[0, par, j, q], got[1, par, j, q]
                    at = 8 * n
                    left = left if at == 0 else pltpu.roll(left, LANES - at, 1)
                    right = right if at == 8 else pltpu.roll(right, (LANES - at + 8) % LANES, 1)
                    edges.append(jnp.where(lane < 8, left, right))
                ehi, elo = split(jnp.concatenate(edges, axis=0))
                hi, lo = split(yb[j, p:p + step].reshape(step * ROWS, LANES))
                value = jnp.dot(jnp.concatenate([hi, lo], axis=1), xm[k], preferred_element_type=jnp.float32)
                value = value + jnp.dot(jnp.concatenate([ehi, elo], axis=1), xe[k], preferred_element_type=jnp.float32)
                value = (value[:, :LANES] + value[:, LANES:]).reshape(step, ROWS, LANES)
                if divide:
                    f[1, j, p:p + step] = moved[p_view, j, p:p + step] / value
                else:
                    f[0, j, p:p + step] = f[0, j, p:p + step] * value

        guarded(even, lambda: body(True))
        guarded(jnp.logical_not(even), lambda: body(False))

        def finish():
            for tc in range(2):
                far_copy, near_copy, local = back(j, tc)
                guarded(local, lambda: near_copy.start())
                guarded(jnp.logical_not(local), lambda: far_copy.start())

        guarded(k < blurs - 1, lambda: send_z(nxt, j))
        guarded(k == blurs - 1, finish)

    def feed(t):
        n = t - (LAG + 2)
        p = 1 + n // (4 * own)
        q = lax.rem(n, 4 * own)
        k = lax.rem(q, 4)
        guarded(jnp.logical_or(away, k > 0), lambda: bulk(p, q // 4, k).start())

    def feed_first(r):
        guarded(away, lambda: bulk(0, r, 0).start())
        for k in range(1, 4):
            bulk(0, r, k).start()

    enter(0)
    enter(1)
    for t in range(LAG + 1):
        if t < own:
            feed_first(t)
        z_stage(t)
        if t:
            y_stage(t - 1)
        if 2 + t < own:
            enter(2 + t)

    def main(t, carry):
        n = t - (LAG + 2)
        guarded(jnp.logical_and(n >= 0, n < 4 * own * (views - 1)), lambda: feed(t))
        z_stage(t)
        y_stage(t - 1)
        x_stage(t - 1 - LAG)
        return carry

    lax.fori_loop(LAG + 1, last, main, 0)
    y_stage(jnp.int32(last - 1))

    def drain(t, carry):
        x_stage(t)
        return carry

    lax.fori_loop(last - 1 - LAG, last, drain, 0)

    def settle(j, carry):
        par = (blurs - 1) % 2
        guarded(has_up, lambda: z_copy(0, par, j).wait_send())
        guarded(has_dn, lambda: z_copy(1, par, j).wait_send())
        for side in range(2):
            guarded(has_r, lambda: x_copy(0, side, j).wait_send())
            guarded(has_l, lambda: x_copy(1, side, j).wait_send())
        for tc in range(2):
            far_copy, near_copy, local = back(j, tc)
            guarded(local, lambda: near_copy.wait())
            guarded(jnp.logical_not(local), lambda: far_copy.wait())
        return carry

    lax.fori_loop(0, chunks, settle, 0)

    def delivered(i, carry):
        p, q = i // (4 * own), lax.rem(i, 4 * own)
        k = lax.rem(q, 4)
        guarded(jnp.logical_or(away, k > 0), lambda: bulk(p, q // 4, k).wait_send())
        return carry

    lax.fori_loop(0, 4 * own * views, delivered, 0)
    for r in range(own):
        guarded(away, lambda: est_copy(r, 0).wait_send())
        for k in range(1, 4):
            est_copy(r, k).wait_send()


def build_weights(views, psf_z, psf_y, psf_x, extents, order, wz, wy, xm, xe):
    def iota(shape, dim):
        return lax.broadcasted_iota(jnp.int32, shape, dim)

    x_which = iota((LANES, LANES), 0) - iota((LANES, LANES), 1) + RL
    r = iota((16, LANES), 0)
    e_which = jnp.where(r < 8, r - 8, r + (LANES - 8)) - iota((16, LANES), 1) + RL
    for p in range(views):
        view = order[p]
        tz = taps_of(psf_z, view, (extents[view, 0] - 1) // 2, RZ)
        ty = taps_of(psf_y, view, (extents[view, 1] - 1) // 2, RL)
        tx = taps_of(psf_x, view, (extents[view, 2] - 1) // 2, RL)
        for i in (2 * p, 2 * p + 1):
            for k in range(2 * RZ + 1):
                wz[i, k] = tz[k]
            for k in range(2 * RL + 1):
                wy[i, k] = ty[k]
            hi, lo = band(tx, x_which)
            for top in (0, LANES):
                xm[i, top:top + LANES, :LANES] = hi
                xm[i, top:top + LANES, LANES:] = lo
            hi, lo = band(tx, e_which)
            xe[i] = jnp.zeros(xe.shape[1:], xe.dtype)
            for top in (0, LANES):
                xe[i, top:top + 16, :LANES] = hi
                xe[i, top:top + 16, LANES:] = lo
            tz, ty, tx = tz[::-1], ty[::-1], tx[::-1]


def slabs(chain, estimate, measured, psf_z, psf_y, psf_x, extents, order):
    views, nz, ny, nx = measured.shape
    planes, rows = 2 * nz, 2 * ny
    chunks, own, blurs = rows // ROWS, ny // ROWS, 2 * views
    f32, bf16 = jnp.float32, jnp.bfloat16
    smem = pl.BlockSpec(memory_space=pltpu.SMEM)
    anywhere = pl.BlockSpec(memory_space=pl.ANY)
    dma = pltpu.SemaphoreType.DMA
    packs = pltpu.VMEM((2, 2, chunks, planes * 8 // LANES, ROWS, LANES), f32)
    return pl.pallas_call(
        functools.partial(wavefront_kernel, chain, nz, ny, views),
        out_shape=jax.ShapeDtypeStruct((nz, ny, nx), f32),
        in_specs=[anywhere] * 2 + [smem] * 5,
        out_specs=anywhere,
        scratch_shapes=[
            pltpu.VMEM((blurs, 2 * RZ + 1, ROWS, LANES), f32),
            pltpu.VMEM((blurs, 2 * RL + 1, ROWS, LANES), f32),
            pltpu.VMEM((blurs, 2 * LANES, 2 * LANES), bf16),
            pltpu.VMEM((blurs, 2 * LANES, 2 * LANES), bf16),
            pltpu.VMEM((2, chunks, planes, ROWS, LANES), f32),
            pltpu.VMEM((2, 2, chunks, RZ, ROWS, LANES), f32),
            pltpu.VMEM((planes, rows + 2 * ROWS, LANES), f32),
            pltpu.VMEM((chunks, planes, ROWS, LANES), f32),
            packs, packs,
            pltpu.VMEM((views, nz, ny, nx), f32),
            pltpu.VMEM((views, nz, ny, nx), f32),
            pltpu.VMEM((views, chunks, planes, ROWS, LANES), f32),
            dma((2, 2, chunks)), dma((2, 2, chunks)),
            dma((2, 2, chunks)), dma((2, 2, chunks)),
            dma((own, 4)), dma((own, 4)),
            dma((views, own, 4)), dma((views, own, 4)),
            dma((own, 4)), dma((own, 4)),
            dma((own,)), dma((own,)), dma,
        ],
        compiler_params=pltpu.CompilerParams(collective_id=1, has_side_effects=True),
    )(estimate, measured, psf_z, psf_y, psf_x, extents, order)


def on_device(estimate, measured, psf_z, psf_y, psf_x, extents, order):
    n_z, n_y = lax.axis_size("gz"), lax.axis_size("gy")
    nz, ny, nx = estimate.shape
    fits = n_y == 2 and n_z % 4 == 0 and nx == 4 * LANES and nz == 16 and 2 * ny == 64
    if fits:
        return slabs(n_z // 2, estimate, measured, psf_z, psf_y, psf_x, extents, order)
    return general(estimate, measured, psf_z, psf_y, psf_x, extents, order)


def solution(mesh):
    return jax.shard_map(
        on_device,
        mesh=mesh,
        in_specs=(P("gz", "gy", None), P(None, "gz", "gy", None), P(), P(), P(), P(), P()),
        out_specs=P("gz", "gy", None),
        check_vma=False,
    )
```

```python
import functools
import jax
import jax.numpy as jnp
from jax import lax
from jax.experimental import pallas as pl
from jax.experimental.pallas import tpu as pltpu
from jax.sharding import PartitionSpec as P

MESH = pl.DeviceIdType.MESH
RZ = 15
RL = 7
LANES = 128


def with_halo(value, sides, width):
    for axis, dim in sides:
        size, length = (lax.axis_size(axis), value.shape[dim])
        up = [(i, (i + 1) % size) for i in range(size - 1)]
        down = [(j, i) for i, j in up]
        last = lax.slice_in_dim(value, length - width, length, axis=dim)
        initial = lax.slice_in_dim(value, 0, width, axis=dim)
        before = lax.ppermute(last, axis, up)
        after = lax.ppermute(initial, axis, down)
        value = jnp.concatenate([before, value, after], axis=dim)
    return value


def line_taps(profile, reach_cells, tap_reach):
    offsets = jnp.arange(2 * tap_reach + 1, dtype=jnp.int32) - tap_reach
    kept = jnp.where(jnp.abs(offsets) <= reach_cells, profile, jnp.zeros_like(profile))
    return kept / jnp.sum(kept)


def correlate_padded(padded, weights, along_axis, tap_reach, length, flipped):
    total = None
    for offset in range(2 * tap_reach + 1):
        start = 2 * tap_reach - offset if flipped else offset
        piece = lax.slice_in_dim(padded, start, start + length, axis=along_axis)
        term = weights[offset] * piece
        total = term if total is None else total + term
    return total


def blur(field, weights_z, weights_y, weights_x, flipped):
    padded = with_halo(field, (("gz", 0),), RZ)
    result = correlate_padded(padded, weights_z, 0, RZ, field.shape[0], flipped)
    widened = with_halo(result, (("gy", 1),), RL)
    result = correlate_padded(widened, weights_y, 1, RL, field.shape[1], flipped)
    result = jnp.pad(result, ((0, 0), (0, 0), (RL, RL)))
    return correlate_padded(result, weights_x, 2, RL, field.shape[2], flipped)


def general(estimate, measured, psf_z, psf_y, psf_x, extents, order):
    current = estimate
    for position in range(measured.shape[0]):
        view = order[position]
        radii = (extents[view] - 1) // 2
        weights_z = line_taps(psf_z[view], radii[0], RZ)
        weights_y = line_taps(psf_y[view], radii[1], RL)
        weights_x = line_taps(psf_x[view], radii[2], RL)
        recorded = lax.dynamic_index_in_dim(measured, view, 0, keepdims=False)
        blurred = blur(current, weights_z, weights_y, weights_x, False)
        ratio = recorded / blurred
        current = current * blur(ratio, weights_z, weights_y, weights_x, True)
    return current


def place():
    g = lax.axis_index("gz")
    w = lax.axis_index("gy")
    return g // 4, (g // 2) % 2, g % 2, w


def slab_of(a, w):
    return 2 * a + lax.rem(w + a, 2)


def group_peers():
    h, a, c, w = place()
    peers = []
    for k in range(1, 8):
        da, dc, dw = k // 4, (k // 2) % 2, k % 2
        device = (4 * h + 2 * lax.rem(a + da, 2) + lax.rem(c + dc, 2), lax.rem(w + dw, 2))
        peers.append(device)
    return peers


def taps_of(profile, view, radius, reach):
    kept = []
    for k in range(2 * reach + 1):
        value = jnp.full((8, LANES), profile[view, k], jnp.float32)
        kept.append(jnp.where(abs(k - reach) <= radius, value, jnp.zeros_like(value)))
    total = kept[0]
    for value in kept[1:]:
        total = total + value
    return [value / total for value in kept]


def band(taps, which):
    total = jnp.zeros(which.shape, jnp.float32)
    for k, tap in enumerate(taps):
        total = jnp.where(which == k, tap[0:1, :], total)
    return split(total)


def split(value):
    hi = value.astype(jnp.bfloat16)
    lo = (value - hi.astype(jnp.float32)).astype(jnp.bfloat16)
    return hi, lo


ROWS = 8
PIECES = 4
GROUPS = 2
WAYS = [(1, -1), (-1, -1), (1, 1), (-1, 1), (0, -1), (0, 1), (1, 0), (-1, 0)]


def wavefront_kernel(chain, nz, ny, views, est, measured, psf_z, psf_y, psf_x, extents, order, out,
                     wz, wy, xm, xe, f, zh, xb, zb, pack, got, stage, chosen, moved,
                     hs, hr, es, er, bs, br, gs, gr, el, gl, fl):
    h, a, c, w = place()
    zi = 2 * h + c
    s = slab_of(a, w)
    planes = 2 * nz
    chunks = 2 * ny // ROWS
    own = ny // ROWS
    home, away = c == a, c != a
    there_z = {1: zi < chain - 1, -1: zi > 0}
    there_x = {1: s < 3, -1: s > 0}

    def there(dz, dx):
        conds = ([there_z[dz]] if dz else []) + ([there_x[dx]] if dx else [])
        return conds[0] if len(conds) == 1 else jnp.logical_and(*conds)

    def device_at(dz, dx):
        z = lax.rem(zi + dz + chain, chain)
        x = lax.rem(s + dx + 4, 4)
        b = x // 2
        return (4 * (z // 2) + 2 * b + lax.rem(z, 2), lax.rem(x + b, 2))

    devices = [device_at(dz, dx) for dz, dx in WAYS]
    sends = [there(dz, dx) for dz, dx in WAYS]
    comes = [there(-dz, -dx) for dz, dx in WAYS]

    def guarded(cond, act):
        @pl.when(cond)
        def _():
            act()

    barrier = pltpu.get_barrier_semaphore()

    def greet(device):
        pl.semaphore_signal(barrier, inc=1, device_id=device, device_id_type=MESH)

    for device in group_peers():
        greet(device)
    count = jnp.int32(7)
    for i, (dz, dx) in enumerate(WAYS):
        if dz:
            other = jnp.logical_and(sends[i], (c == 1) if dz > 0 else (c == 0))
            guarded(other, lambda: greet(devices[i]))
            count = count + other.astype(jnp.int32)
    fetch = pltpu.make_async_copy(measured, stage, fl)
    fetch.start()
    pl.semaphore_wait(barrier, count)

    def remote(src, dst, send, recv, device):
        return pltpu.make_async_remote_copy(src_ref=src, dst_ref=dst, send_sem=send, recv_sem=recv,
                                            device_id=device, device_id_type=MESH)

    def outward(r, k):
        da, dw = k // 2, k % 2
        ta, tw = lax.rem(c + da, 2), lax.rem(w + dw, 2)
        x0 = pl.multiple_of(LANES * slab_of(ta, tw), LANES)
        return ((slice(None), pl.ds(ROWS * r, ROWS), pl.ds(x0, LANES)),
                (own * w + r, pl.ds(nz * c, nz)), (4 * h + 2 * ta + a, tw))

    def est_copy(r, k):
        src, dst, device = outward(r, k)
        return remote(est.at[src], f.at[(0,) + dst], es.at[r, k], er.at[r, k], device)

    def est_local(r):
        src, dst, _ = outward(r, 0)
        return pltpu.make_async_copy(est.at[src], f.at[(0,) + dst], el.at[r])

    def bulk(p, r, k):
        src, dst, device = outward(r, k)
        return remote(chosen.at[(p,) + src], moved.at[(p,) + dst], bs.at[p, r, k], br.at[p, r, k], device)

    def bulk_start(p, r, u, on=None):
        k = 2 * (u // 2) + lax.rem(u % 2 + away.astype(jnp.int32), 2)
        real = jnp.logical_or(away, k > 0)
        guarded(real if on is None else jnp.logical_and(real, on), lambda: bulk(p, r, k).start())

    def back(j, tc):
        tw, r = j // own, j % own
        k = 2 * lax.rem(tc + a, 2) + lax.rem(tw + w, 2)
        x0 = pl.multiple_of(LANES * s, LANES)
        src = f.at[0, j, pl.ds(nz * tc, nz)]
        dst = out.at[:, pl.ds(ROWS * r, ROWS), pl.ds(x0, LANES)]
        return (remote(src, dst, gs.at[r, k], gr.at[r, k], (4 * h + 2 * c + tc, tw)),
                pltpu.make_async_copy(src, dst, gl.at[r]), jnp.logical_and(home, k == 0))

    def halo(i, par, j):
        dz, dx = WAYS[i]
        if dx == 0:
            src = f.at[par, j, pl.ds(planes - RZ if dz > 0 else 0, RZ)]
            dst = zh.at[0 if dz > 0 else 1, par, j]
        else:
            mine, theirs = (0, 1) if dx < 0 else (1, 0)
            if dz == 0:
                src, dst = pack.at[mine, par, j], got.at[theirs, par, j, pl.ds(1, 2)]
            elif dz > 0:
                src, dst = pack.at[mine, par, j, pl.ds(1, 1)], got.at[theirs, par, j, pl.ds(0, 1)]
            else:
                src, dst = pack.at[mine, par, j, pl.ds(0, 1)], got.at[theirs, par, j, pl.ds(3, 1)]
        return remote(src, dst, hs.at[i, par, j], hr.at[i, par, j], devices[i])

    def emit(par, j, on=None):
        for i in range(len(WAYS)):
            cond = sends[i] if on is None else jnp.logical_and(sends[i], on)
            guarded(cond, lambda: halo(i, par, j).start())

    def arrive(par, j):
        for i in range(len(WAYS)):
            guarded(comes[i], lambda: halo(i, par, j).wait_recv())

    def gone(par, j, on=None):
        for i in range(len(WAYS)):
            cond = sends[i] if on is None else jnp.logical_and(sends[i], on)
            guarded(cond, lambda: halo(i, par, j).wait_send())

    for r in range(own):
        for k in range(1, 4):
            est_copy(r, k).start()
        guarded(away, lambda: est_copy(r, 0).start())
        guarded(home, lambda: est_local(r).start())

    build_weights(views, psf_z, psf_y, psf_x, extents, order, wz, wy, xm, xe)

    zb[...] = jnp.zeros_like(zb)

    def clear(ref, side):
        def one(i, carry):
            ref[side, i // chunks, lax.rem(i, chunks)] = jnp.zeros(ref.shape[3:], jnp.float32)
            return carry

        lax.fori_loop(0, 2 * chunks, one, 0)

    def clear_corner(q):
        def one(i, carry):
            for side in range(2):
                got[side, i // chunks, lax.rem(i, chunks), q] = jnp.zeros((ROWS, LANES), jnp.float32)
            return carry

        lax.fori_loop(0, 2 * chunks, one, 0)

    for side, d in ((0, -1), (1, 1)):
        guarded(jnp.logical_not(there_z[d]), lambda: clear(zh, side))
        guarded(jnp.logical_not(there_z[d]), lambda: clear_corner(3 * side))
        guarded(jnp.logical_not(there_x[d]), lambda: clear(got, side))

    fetch.wait()
    for p in range(views):
        def pick(i, carry):
            chosen[p, i] = stage[order[p], i]
            return carry

        lax.fori_loop(0, nz, pick, 0)

    def keep():
        x0 = pl.multiple_of(LANES * slab_of(c, w), LANES)
        for p in range(views):
            for r in range(own):
                moved[p, own * w + r, pl.ds(nz * c, nz)] = chosen[p, :, r * ROWS:(r + 1) * ROWS, pl.ds(x0, LANES)]

    guarded(home, keep)

    lane = lax.broadcasted_iota(jnp.int32, (ROWS, LANES), 1)
    per = LANES // 8
    half = 16

    def pack_edges(values, par, j):
        for q in range(planes // per):
            packed_l = packed_r = None
            for i in range(per):
                value = values[q * per + i]
                at = 8 * i
                left = value if at == 0 else pltpu.roll(value, at, 1)
                right = pltpu.roll(value, (at + 8) % LANES, 1) if at + 8 < LANES else value
                packed_l = left if packed_l is None else jnp.where(lane >= at, left, packed_l)
                packed_r = right if packed_r is None else jnp.where(lane >= at, right, packed_r)
            pack[0, par, j, q] = packed_l
            pack[1, par, j, q] = packed_r

    def enter(i):
        guarded(home, lambda: est_local(i).wait())
        guarded(away, lambda: est_copy(i, 0).wait_recv())
        for k in range(1, 4):
            est_copy(i, k).wait_recv()
        for j in (i, i + own):
            pack_edges([f[0, j, p] for p in range(planes)], 0, j)
            emit(0, j)

    wide = planes + 2 * RZ

    def x_stage(k, par, j):
        rows = jnp.concatenate([zh[0, par, j].reshape(RZ * ROWS, LANES), f[par, j].reshape(planes * ROWS, LANES),
                                zh[1, par, j].reshape(RZ * ROWS, LANES)], axis=0)
        m = wide // GROUPS
        for g in range(GROUPS):
            edges = []
            for i in range(m):
                q, n = divmod(g * m + i + 1, per)
                left, right = got[0, par, j, q], got[1, par, j, q]
                at = 8 * n
                left = left if at == 0 else pltpu.roll(left, LANES - at, 1)
                right = right if at == 8 else pltpu.roll(right, (LANES - at + 8) % LANES, 1)
                edges.append(jnp.where(lane < 8, left, right))
            ehi, elo = split(jnp.concatenate(edges, axis=0))
            hi, lo = split(rows[g * m * ROWS:(g + 1) * m * ROWS])
            value = jnp.dot(jnp.concatenate([hi, lo], axis=1), xm[k], preferred_element_type=jnp.float32)
            value = value + jnp.dot(jnp.concatenate([ehi, elo], axis=1), xe[k], preferred_element_type=jnp.float32)
            xb[j % 2, g * m:(g + 1) * m] = (value[:, :LANES] + value[:, LANES:]).reshape(m, ROWS, LANES)

    def z_stage(k, j):
        taps = [wz[k, i] for i in range(2 * RZ + 1)]
        for first in range(0, planes, half):
            acc = [None] * half
            for p in range(first, first + half + 2 * RZ):
                v = xb[j % 2, p]
                for o in range(half):
                    i = p - first - o
                    if 0 <= i <= 2 * RZ:
                        term = taps[i] * v
                        acc[o] = term if acc[o] is None else acc[o] + term
            for o in range(half):
                zb[first + o, ROWS * (j + 1):ROWS * (j + 2), :] = acc[o]

    def y_stage(k, view, odd, j):
        taps = [wy[k, i] for i in range(2 * RL + 1)]
        base = ROWS * (j + 1) - RL
        values = []
        for p in range(planes):
            value = None
            for o in range(2 * RL + 1):
                term = taps[o] * zb[p, base + o:base + o + ROWS, :]
                value = term if value is None else value + term
            value = f[0, j, p] * value if odd else moved[view, j, p] / value
            f[0 if odd else 1, j, p] = value
            values.append(value)
        pack_edges(values, 0 if odd else 1, j)

    def y_waits(view, odd, j, on):
        gone(0 if odd else 1, j, on)
        if not odd:
            dw = lax.rem(w + j // own, 2)
            r = j % own
            guarded(jnp.logical_or(away, dw > 0), lambda: bulk(view, r, dw).wait_recv())
            bulk(view, r, 2 + dw).wait_recv()

    def finish(j):
        for tc in range(2):
            far_copy, near_copy, local = back(j, tc)
            guarded(local, lambda: near_copy.start())
            guarded(jnp.logical_not(local), lambda: far_copy.start())

    for i in range(own):
        enter(i)
    for r in range(own):
        for u in range(PIECES):
            bulk_start(0, r, u)

    steps = 2 * chunks

    def one_view(view, carry):
        for i in range(steps):
            e, j = divmod(i, chunks)
            oy, jy = divmod((i - 2) % steps, chunks)
            r, u = divmod((i - 2) % steps, PIECES)
            arrive(e, j)
            if i >= 2:
                y_waits(view, oy, jy, None if oy else view > 0)
                x_stage(2 * view + e, e, j)
                y_stage(2 * view + oy, view, oy, jy)
                emit(1 - oy, jy, view < views - 1 if oy else None)
                if oy:
                    guarded(view == views - 1, lambda: finish(jy))
                bulk_start(view + 1, r, u, view < views - 1)
            else:
                x_stage(2 * view + e, e, j)

                def before():
                    y_waits(view - 1, 1, jy, None)
                    y_stage(2 * view - 1, view - 1, 1, jy)
                    emit(0, jy)
                    bulk_start(view, r, u)

                guarded(view > 0, before)
            z_stage(2 * view + e, j)
        return carry

    lax.fori_loop(0, views, one_view, 0)
    for jy in (chunks - 2, chunks - 1):
        y_waits(views - 1, 1, jy, None)
        y_stage(2 * views - 1, views - 1, 1, jy)
        finish(jy)

    for j in range(chunks):
        gone(1, j)
        for tc in range(2):
            far_copy, near_copy, local = back(j, tc)
            guarded(local, lambda: near_copy.wait())
            guarded(jnp.logical_not(local), lambda: far_copy.wait())
    for r in range(own):
        guarded(away, lambda: est_copy(r, 0).wait_send())
        for k in range(1, 4):
            est_copy(r, k).wait_send()

    def delivered(p, carry):
        for r in range(own):
            guarded(away, lambda: bulk(p, r, 0).wait_send())
            for k in range(1, 4):
                bulk(p, r, k).wait_send()
        return carry

    lax.fori_loop(0, views, delivered, 0)


def build_weights(views, psf_z, psf_y, psf_x, extents, order, wz, wy, xm, xe):
    def iota(shape, dim):
        return lax.broadcasted_iota(jnp.int32, shape, dim)

    x_which = iota((LANES, LANES), 0) - iota((LANES, LANES), 1) + RL
    r = iota((16, LANES), 0)
    e_which = jnp.where(r < 8, r - 8, r + (LANES - 8)) - iota((16, LANES), 1) + RL
    for p in range(views):
        view = order[p]
        tz = taps_of(psf_z, view, (extents[view, 0] - 1) // 2, RZ)
        ty = taps_of(psf_y, view, (extents[view, 1] - 1) // 2, RL)
        tx = taps_of(psf_x, view, (extents[view, 2] - 1) // 2, RL)
        for i in (2 * p, 2 * p + 1):
            for k in range(2 * RZ + 1):
                wz[i, k] = tz[k]
            for k in range(2 * RL + 1):
                wy[i, k] = ty[k]
            hi, lo = band(tx, x_which)
            for top in (0, LANES):
                xm[i, top:top + LANES, :LANES] = hi
                xm[i, top:top + LANES, LANES:] = lo
            hi, lo = band(tx, e_which)
            xe[i] = jnp.zeros(xe.shape[1:], xe.dtype)
            for top in (0, LANES):
                xe[i, top:top + 16, :LANES] = hi
                xe[i, top:top + 16, LANES:] = lo
            tz, ty, tx = tz[::-1], ty[::-1], tx[::-1]


def slabs(chain, estimate, measured, psf_z, psf_y, psf_x, extents, order):
    views, nz, ny, nx = measured.shape
    planes, rows = 2 * nz, 2 * ny
    chunks, own, blurs = rows // ROWS, ny // ROWS, 2 * views
    f32, bf16 = jnp.float32, jnp.bfloat16
    smem = pl.BlockSpec(memory_space=pltpu.SMEM)
    anywhere = pl.BlockSpec(memory_space=pl.ANY)
    dma = pltpu.SemaphoreType.DMA
    ways = len(WAYS)
    packed = planes * 8 // LANES
    return pl.pallas_call(
        functools.partial(wavefront_kernel, chain, nz, ny, views),
        out_shape=jax.ShapeDtypeStruct((nz, ny, nx), f32),
        in_specs=[anywhere] * 2 + [smem] * 5,
        out_specs=anywhere,
        scratch_shapes=[
            pltpu.VMEM((blurs, 2 * RZ + 1, ROWS, LANES), f32),
            pltpu.VMEM((blurs, 2 * RL + 1, ROWS, LANES), f32),
            pltpu.VMEM((blurs, 2 * LANES, 2 * LANES), bf16),
            pltpu.VMEM((blurs, 2 * LANES, 2 * LANES), bf16),
            pltpu.VMEM((2, chunks, planes, ROWS, LANES), f32),
            pltpu.VMEM((2, 2, chunks, RZ, ROWS, LANES), f32),
            pltpu.VMEM((2, planes + 2 * RZ, ROWS, LANES), f32),
            pltpu.VMEM((planes, rows + 2 * ROWS, LANES), f32),
            pltpu.VMEM((2, 2, chunks, packed, ROWS, LANES), f32),
            pltpu.VMEM((2, 2, chunks, packed + 2, ROWS, LANES), f32),
            pltpu.VMEM((views, nz, ny, nx), f32),
            pltpu.VMEM((views, nz, ny, nx), f32),
            pltpu.VMEM((views, chunks, planes, ROWS, LANES), f32),
            dma((ways, 2, chunks)), dma((ways, 2, chunks)),
            dma((own, 4)), dma((own, 4)),
            dma((views, own, 4)), dma((views, own, 4)),
            dma((own, 4)), dma((own, 4)),
            dma((own,)), dma((own,)), dma,
        ],
        compiler_params=pltpu.CompilerParams(collective_id=1, has_side_effects=True),
    )(estimate, measured, psf_z, psf_y, psf_x, extents, order)


def on_device(estimate, measured, psf_z, psf_y, psf_x, extents, order):
    n_z, n_y = lax.axis_size("gz"), lax.axis_size("gy")
    nz, ny, nx = estimate.shape
    fits = n_y == 2 and n_z % 4 == 0 and nx == 4 * LANES and nz == 16 and 2 * ny == 64
    if fits:
        return slabs(n_z // 2, estimate, measured, psf_z, psf_y, psf_x, extents, order)
    return general(estimate, measured, psf_z, psf_y, psf_x, extents, order)


def solution(mesh):
    return jax.shard_map(
        on_device,
        mesh=mesh,
        in_specs=(P("gz", "gy", None), P(None, "gz", "gy", None), P(), P(), P(), P(), P()),
        out_specs=P("gz", "gy", None),
        check_vma=False,
    )
```

```python
import functools
import jax
import jax.numpy as jnp
from jax import lax
from jax.experimental import pallas as pl
from jax.experimental.pallas import tpu as pltpu
from jax.sharding import PartitionSpec as P

MESH = pl.DeviceIdType.MESH
RZ = 15
RL = 7
LANES = 128


def with_halo(value, sides, width):
    for axis, dim in sides:
        size, length = (lax.axis_size(axis), value.shape[dim])
        up = [(i, (i + 1) % size) for i in range(size - 1)]
        down = [(j, i) for i, j in up]
        last = lax.slice_in_dim(value, length - width, length, axis=dim)
        initial = lax.slice_in_dim(value, 0, width, axis=dim)
        before = lax.ppermute(last, axis, up)
        after = lax.ppermute(initial, axis, down)
        value = jnp.concatenate([before, value, after], axis=dim)
    return value


def line_taps(profile, reach_cells, tap_reach):
    offsets = jnp.arange(2 * tap_reach + 1, dtype=jnp.int32) - tap_reach
    kept = jnp.where(jnp.abs(offsets) <= reach_cells, profile, jnp.zeros_like(profile))
    return kept / jnp.sum(kept)


def correlate_padded(padded, weights, along_axis, tap_reach, length, flipped):
    total = None
    for offset in range(2 * tap_reach + 1):
        start = 2 * tap_reach - offset if flipped else offset
        piece = lax.slice_in_dim(padded, start, start + length, axis=along_axis)
        term = weights[offset] * piece
        total = term if total is None else total + term
    return total


def blur(field, weights_z, weights_y, weights_x, flipped):
    padded = with_halo(field, (("gz", 0),), RZ)
    result = correlate_padded(padded, weights_z, 0, RZ, field.shape[0], flipped)
    widened = with_halo(result, (("gy", 1),), RL)
    result = correlate_padded(widened, weights_y, 1, RL, field.shape[1], flipped)
    result = jnp.pad(result, ((0, 0), (0, 0), (RL, RL)))
    return correlate_padded(result, weights_x, 2, RL, field.shape[2], flipped)


def general(estimate, measured, psf_z, psf_y, psf_x, extents, order):
    current = estimate
    for position in range(measured.shape[0]):
        view = order[position]
        radii = (extents[view] - 1) // 2
        weights_z = line_taps(psf_z[view], radii[0], RZ)
        weights_y = line_taps(psf_y[view], radii[1], RL)
        weights_x = line_taps(psf_x[view], radii[2], RL)
        recorded = lax.dynamic_index_in_dim(measured, view, 0, keepdims=False)
        blurred = blur(current, weights_z, weights_y, weights_x, False)
        ratio = recorded / blurred
        current = current * blur(ratio, weights_z, weights_y, weights_x, True)
    return current


def place():
    g = lax.axis_index("gz")
    w = lax.axis_index("gy")
    return g // 4, (g // 2) % 2, g % 2, w


def slab_of(a, w):
    return 2 * a + lax.rem(w + a, 2)


def group_peers():
    h, a, c, w = place()
    peers = []
    for k in range(1, 8):
        da, dc, dw = k // 4, (k // 2) % 2, k % 2
        device = (4 * h + 2 * lax.rem(a + da, 2) + lax.rem(c + dc, 2), lax.rem(w + dw, 2))
        peers.append(device)
    return peers


def taps_of(profile, view, radius, reach):
    kept = []
    for k in range(2 * reach + 1):
        value = jnp.full((8, LANES), profile[view, k], jnp.float32)
        kept.append(jnp.where(abs(k - reach) <= radius, value, jnp.zeros_like(value)))
    total = kept[0]
    for value in kept[1:]:
        total = total + value
    return [value / total for value in kept]


def band(taps, which):
    total = jnp.zeros(which.shape, jnp.float32)
    for k, tap in enumerate(taps):
        total = jnp.where(which == k, tap[0:1, :], total)
    return split(total)


def split(value):
    hi = value.astype(jnp.bfloat16)
    lo = (value - hi.astype(jnp.float32)).astype(jnp.bfloat16)
    return hi, lo


ROWS = 8
PIECES = 4
GROUPS = 1
WAYS = [(1, -1), (-1, -1), (1, 1), (-1, 1), (0, -1), (0, 1), (1, 0), (-1, 0)]


def wavefront_kernel(chain, nz, ny, views, est, measured, psf_z, psf_y, psf_x, extents, order, out,
                     wz, wy, xm, xe, f, zh, xb, zb, pack, got, stage, chosen, moved,
                     hs, hr, es, er, bs, br, gs, gr, el, gl, fl):
    h, a, c, w = place()
    zi = 2 * h + c
    s = slab_of(a, w)
    planes = 2 * nz
    chunks = 2 * ny // ROWS
    own = ny // ROWS
    home, away = c == a, c != a
    there_z = {1: zi < chain - 1, -1: zi > 0}
    there_x = {1: s < 3, -1: s > 0}

    def there(dz, dx):
        conds = ([there_z[dz]] if dz else []) + ([there_x[dx]] if dx else [])
        return conds[0] if len(conds) == 1 else jnp.logical_and(*conds)

    def device_at(dz, dx):
        z = lax.rem(zi + dz + chain, chain)
        x = lax.rem(s + dx + 4, 4)
        b = x // 2
        return (4 * (z // 2) + 2 * b + lax.rem(z, 2), lax.rem(x + b, 2))

    devices = [device_at(dz, dx) for dz, dx in WAYS]
    sends = [there(dz, dx) for dz, dx in WAYS]
    comes = [there(-dz, -dx) for dz, dx in WAYS]

    def guarded(cond, act):
        @pl.when(cond)
        def _():
            act()

    barrier = pltpu.get_barrier_semaphore()

    def greet(device):
        pl.semaphore_signal(barrier, inc=1, device_id=device, device_id_type=MESH)

    for device in group_peers():
        greet(device)
    count = jnp.int32(7)
    for i, (dz, dx) in enumerate(WAYS):
        if dz:
            other = jnp.logical_and(sends[i], (c == 1) if dz > 0 else (c == 0))
            guarded(other, lambda: greet(devices[i]))
            count = count + other.astype(jnp.int32)
    fetch = pltpu.make_async_copy(measured, stage, fl)
    fetch.start()
    pl.semaphore_wait(barrier, count)

    def remote(src, dst, send, recv, device):
        return pltpu.make_async_remote_copy(src_ref=src, dst_ref=dst, send_sem=send, recv_sem=recv,
                                            device_id=device, device_id_type=MESH)

    def outward(r, k):
        da, dw = k // 2, k % 2
        ta, tw = lax.rem(c + da, 2), lax.rem(w + dw, 2)
        x0 = pl.multiple_of(LANES * slab_of(ta, tw), LANES)
        return ((slice(None), pl.ds(ROWS * r, ROWS), pl.ds(x0, LANES)),
                (own * w + r, pl.ds(nz * c, nz)), (4 * h + 2 * ta + a, tw))

    def est_copy(r, k):
        src, dst, device = outward(r, k)
        return remote(est.at[src], f.at[(0,) + dst], es.at[r, k], er.at[r, k], device)

    def est_local(r):
        src, dst, _ = outward(r, 0)
        return pltpu.make_async_copy(est.at[src], f.at[(0,) + dst], el.at[r])

    def bulk(p, r, k):
        src, dst, device = outward(r, k)
        return remote(chosen.at[(p,) + src], moved.at[(p,) + dst], bs.at[p, r, k], br.at[p, r, k], device)

    def bulk_start(p, r, u, on=None):
        k = 2 * (u // 2) + lax.rem(u % 2 + away.astype(jnp.int32), 2)
        real = jnp.logical_or(away, k > 0)
        guarded(real if on is None else jnp.logical_and(real, on), lambda: bulk(p, r, k).start())

    def back(j, tc):
        tw, r = j // own, j % own
        k = 2 * lax.rem(tc + a, 2) + lax.rem(tw + w, 2)
        x0 = pl.multiple_of(LANES * s, LANES)
        src = f.at[0, j, pl.ds(nz * tc, nz)]
        dst = out.at[:, pl.ds(ROWS * r, ROWS), pl.ds(x0, LANES)]
        return (remote(src, dst, gs.at[r, k], gr.at[r, k], (4 * h + 2 * c + tc, tw)),
                pltpu.make_async_copy(src, dst, gl.at[r]), jnp.logical_and(home, k == 0))

    def halo(i, par, j):
        dz, dx = WAYS[i]
        if dx == 0:
            src = f.at[par, j, pl.ds(planes - RZ if dz > 0 else 0, RZ)]
            dst = zh.at[0 if dz > 0 else 1, par, j]
        else:
            mine, theirs = (0, 1) if dx < 0 else (1, 0)
            if dz == 0:
                src, dst = pack.at[mine, par, j], got.at[theirs, par, j, pl.ds(1, 2)]
            elif dz > 0:
                src, dst = pack.at[mine, par, j, pl.ds(1, 1)], got.at[theirs, par, j, pl.ds(0, 1)]
            else:
                src, dst = pack.at[mine, par, j, pl.ds(0, 1)], got.at[theirs, par, j, pl.ds(3, 1)]
        return remote(src, dst, hs.at[i, par, j], hr.at[i, par, j], devices[i])

    def emit(par, j, on=None):
        for i in range(len(WAYS)):
            cond = sends[i] if on is None else jnp.logical_and(sends[i], on)
            guarded(cond, lambda: halo(i, par, j).start())

    def arrive(par, j):
        for i in range(len(WAYS)):
            guarded(comes[i], lambda: halo(i, par, j).wait_recv())

    def gone(par, j, on=None):
        for i in range(len(WAYS)):
            cond = sends[i] if on is None else jnp.logical_and(sends[i], on)
            guarded(cond, lambda: halo(i, par, j).wait_send())

    for r in range(own):
        for k in range(1, 4):
            est_copy(r, k).start()
        guarded(away, lambda: est_copy(r, 0).start())
        guarded(home, lambda: est_local(r).start())

    build_weights(views, psf_z, psf_y, psf_x, extents, order, wz, wy, xm, xe)

    zb[...] = jnp.zeros_like(zb)

    def clear(ref, side):
        def one(i, carry):
            ref[side, i // chunks, lax.rem(i, chunks)] = jnp.zeros(ref.shape[3:], jnp.float32)
            return carry

        lax.fori_loop(0, 2 * chunks, one, 0)

    def clear_corner(q):
        def one(i, carry):
            for side in range(2):
                got[side, i // chunks, lax.rem(i, chunks), q] = jnp.zeros((ROWS, LANES), jnp.float32)
            return carry

        lax.fori_loop(0, 2 * chunks, one, 0)

    for side, d in ((0, -1), (1, 1)):
        guarded(jnp.logical_not(there_z[d]), lambda: clear(zh, side))
        guarded(jnp.logical_not(there_z[d]), lambda: clear_corner(3 * side))
        guarded(jnp.logical_not(there_x[d]), lambda: clear(got, side))

    fetch.wait()
    for p in range(views):
        def pick(i, carry):
            chosen[p, i] = stage[order[p], i]
            return carry

        lax.fori_loop(0, nz, pick, 0)

    def keep():
        x0 = pl.multiple_of(LANES * slab_of(c, w), LANES)
        for p in range(views):
            for r in range(own):
                moved[p, own * w + r, pl.ds(nz * c, nz)] = chosen[p, :, r * ROWS:(r + 1) * ROWS, pl.ds(x0, LANES)]

    guarded(home, keep)

    lane = lax.broadcasted_iota(jnp.int32, (ROWS, LANES), 1)
    per = LANES // 8
    half = 16

    def pack_edges(values, par, j):
        for q in range(planes // per):
            packed_l = packed_r = None
            for i in range(per):
                value = values[q * per + i]
                at = 8 * i
                left = value if at == 0 else pltpu.roll(value, at, 1)
                right = pltpu.roll(value, (at + 8) % LANES, 1) if at + 8 < LANES else value
                packed_l = left if packed_l is None else jnp.where(lane >= at, left, packed_l)
                packed_r = right if packed_r is None else jnp.where(lane >= at, right, packed_r)
            pack[0, par, j, q] = packed_l
            pack[1, par, j, q] = packed_r

    def enter(i):
        guarded(home, lambda: est_local(i).wait())
        guarded(away, lambda: est_copy(i, 0).wait_recv())
        for k in range(1, 4):
            est_copy(i, k).wait_recv()
        for j in (i, i + own):
            pack_edges([f[0, j, p] for p in range(planes)], 0, j)
            emit(0, j)

    wide = planes + 2 * RZ

    def x_stage(k, par, j):
        rows = jnp.concatenate([zh[0, par, j].reshape(RZ * ROWS, LANES), f[par, j].reshape(planes * ROWS, LANES),
                                zh[1, par, j].reshape(RZ * ROWS, LANES)], axis=0)
        m = wide // GROUPS
        for g in range(GROUPS):
            edges = []
            for i in range(m):
                q, n = divmod(g * m + i + 1, per)
                left, right = got[0, par, j, q], got[1, par, j, q]
                at = 8 * n
                left = left if at == 0 else pltpu.roll(left, LANES - at, 1)
                right = right if at == 8 else pltpu.roll(right, (LANES - at + 8) % LANES, 1)
                edges.append(jnp.where(lane < 8, left, right))
            ehi, elo = split(jnp.concatenate(edges, axis=0))
            hi, lo = split(rows[g * m * ROWS:(g + 1) * m * ROWS])
            value = jnp.dot(jnp.concatenate([hi, lo], axis=1), xm[k], preferred_element_type=jnp.float32)
            value = value + jnp.dot(jnp.concatenate([ehi, elo], axis=1), xe[k], preferred_element_type=jnp.float32)
            xb[j % 2, g * m:(g + 1) * m] = (value[:, :LANES] + value[:, LANES:]).reshape(m, ROWS, LANES)

    def z_stage(k, j):
        taps = [wz[k, i] for i in range(2 * RZ + 1)]
        for first in range(0, planes, half):
            acc = [None] * half
            for p in range(first, first + half + 2 * RZ):
                v = xb[j % 2, p]
                for o in range(half):
                    i = p - first - o
                    if 0 <= i <= 2 * RZ:
                        term = taps[i] * v
                        acc[o] = term if acc[o] is None else acc[o] + term
            for o in range(half):
                zb[first + o, ROWS * (j + 1):ROWS * (j + 2), :] = acc[o]

    def y_stage(k, view, odd, j):
        taps = [wy[k, i] for i in range(2 * RL + 1)]
        base = ROWS * (j + 1) - RL
        values = []
        for p in range(planes):
            value = None
            for o in range(2 * RL + 1):
                term = taps[o] * zb[p, base + o:base + o + ROWS, :]
                value = term if value is None else value + term
            value = f[0, j, p] * value if odd else moved[view, j, p] / value
            f[0 if odd else 1, j, p] = value
            values.append(value)
        pack_edges(values, 0 if odd else 1, j)

    def y_waits(view, odd, j, on):
        gone(0 if odd else 1, j, on)
        if not odd:
            dw = lax.rem(w + j // own, 2)
            r = j % own
            guarded(jnp.logical_or(away, dw > 0), lambda: bulk(view, r, dw).wait_recv())
            bulk(view, r, 2 + dw).wait_recv()

    def finish(j):
        for tc in range(2):
            far_copy, near_copy, local = back(j, tc)
            guarded(local, lambda: near_copy.start())
            guarded(jnp.logical_not(local), lambda: far_copy.start())

    for i in range(own):
        enter(i)
    for r in range(own):
        for u in range(PIECES):
            bulk_start(0, r, u)

    steps = 2 * chunks

    def one_view(view, carry):
        for i in range(steps):
            e, j = divmod(i, chunks)
            oy, jy = divmod((i - 2) % steps, chunks)
            r, u = divmod((i - 2) % steps, PIECES)
            arrive(e, j)
            if i >= 2:
                y_waits(view, oy, jy, None if oy else view > 0)
                x_stage(2 * view + e, e, j)
                y_stage(2 * view + oy, view, oy, jy)
                emit(1 - oy, jy, view < views - 1 if oy else None)
                if oy:
                    guarded(view == views - 1, lambda: finish(jy))
                bulk_start(view + 1, r, u, view < views - 1)
            else:
                x_stage(2 * view + e, e, j)

                def before():
                    y_waits(view - 1, 1, jy, None)
                    y_stage(2 * view - 1, view - 1, 1, jy)
                    emit(0, jy)
                    bulk_start(view, r, u)

                guarded(view > 0, before)
            z_stage(2 * view + e, j)
        return carry

    lax.fori_loop(0, views, one_view, 0)
    for jy in (chunks - 2, chunks - 1):
        y_waits(views - 1, 1, jy, None)
        y_stage(2 * views - 1, views - 1, 1, jy)
        finish(jy)

    for j in range(chunks):
        gone(1, j)
        for tc in range(2):
            far_copy, near_copy, local = back(j, tc)
            guarded(local, lambda: near_copy.wait())
            guarded(jnp.logical_not(local), lambda: far_copy.wait())
    for r in range(own):
        guarded(away, lambda: est_copy(r, 0).wait_send())
        for k in range(1, 4):
            est_copy(r, k).wait_send()

    def delivered(p, carry):
        for r in range(own):
            guarded(away, lambda: bulk(p, r, 0).wait_send())
            for k in range(1, 4):
                bulk(p, r, k).wait_send()
        return carry

    lax.fori_loop(0, views, delivered, 0)


def build_weights(views, psf_z, psf_y, psf_x, extents, order, wz, wy, xm, xe):
    def iota(shape, dim):
        return lax.broadcasted_iota(jnp.int32, shape, dim)

    x_which = iota((LANES, LANES), 0) - iota((LANES, LANES), 1) + RL
    r = iota((16, LANES), 0)
    e_which = jnp.where(r < 8, r - 8, r + (LANES - 8)) - iota((16, LANES), 1) + RL
    for p in range(views):
        view = order[p]
        tz = taps_of(psf_z, view, (extents[view, 0] - 1) // 2, RZ)
        ty = taps_of(psf_y, view, (extents[view, 1] - 1) // 2, RL)
        tx = taps_of(psf_x, view, (extents[view, 2] - 1) // 2, RL)
        for i in (2 * p, 2 * p + 1):
            for k in range(2 * RZ + 1):
                wz[i, k] = tz[k]
            for k in range(2 * RL + 1):
                wy[i, k] = ty[k]
            hi, lo = band(tx, x_which)
            for top in (0, LANES):
                xm[i, top:top + LANES, :LANES] = hi
                xm[i, top:top + LANES, LANES:] = lo
            hi, lo = band(tx, e_which)
            xe[i] = jnp.zeros(xe.shape[1:], xe.dtype)
            for top in (0, LANES):
                xe[i, top:top + 16, :LANES] = hi
                xe[i, top:top + 16, LANES:] = lo
            tz, ty, tx = tz[::-1], ty[::-1], tx[::-1]


def slabs(chain, estimate, measured, psf_z, psf_y, psf_x, extents, order):
    views, nz, ny, nx = measured.shape
    planes, rows = 2 * nz, 2 * ny
    chunks, own, blurs = rows // ROWS, ny // ROWS, 2 * views
    f32, bf16 = jnp.float32, jnp.bfloat16
    smem = pl.BlockSpec(memory_space=pltpu.SMEM)
    anywhere = pl.BlockSpec(memory_space=pl.ANY)
    dma = pltpu.SemaphoreType.DMA
    ways = len(WAYS)
    packed = planes * 8 // LANES
    return pl.pallas_call(
        functools.partial(wavefront_kernel, chain, nz, ny, views),
        out_shape=jax.ShapeDtypeStruct((nz, ny, nx), f32),
        in_specs=[anywhere] * 2 + [smem] * 5,
        out_specs=anywhere,
        scratch_shapes=[
            pltpu.VMEM((blurs, 2 * RZ + 1, ROWS, LANES), f32),
            pltpu.VMEM((blurs, 2 * RL + 1, ROWS, LANES), f32),
            pltpu.VMEM((blurs, 2 * LANES, 2 * LANES), bf16),
            pltpu.VMEM((blurs, 2 * LANES, 2 * LANES), bf16),
            pltpu.VMEM((2, chunks, planes, ROWS, LANES), f32),
            pltpu.VMEM((2, 2, chunks, RZ, ROWS, LANES), f32),
            pltpu.VMEM((2, planes + 2 * RZ, ROWS, LANES), f32),
            pltpu.VMEM((planes, rows + 2 * ROWS, LANES), f32),
            pltpu.VMEM((2, 2, chunks, packed, ROWS, LANES), f32),
            pltpu.VMEM((2, 2, chunks, packed + 2, ROWS, LANES), f32),
            pltpu.VMEM((views, nz, ny, nx), f32),
            pltpu.VMEM((views, nz, ny, nx), f32),
            pltpu.VMEM((views, chunks, planes, ROWS, LANES), f32),
            dma((ways, 2, chunks)), dma((ways, 2, chunks)),
            dma((own, 4)), dma((own, 4)),
            dma((views, own, 4)), dma((views, own, 4)),
            dma((own, 4)), dma((own, 4)),
            dma((own,)), dma((own,)), dma,
        ],
        compiler_params=pltpu.CompilerParams(collective_id=1, has_side_effects=True),
    )(estimate, measured, psf_z, psf_y, psf_x, extents, order)


def on_device(estimate, measured, psf_z, psf_y, psf_x, extents, order):
    n_z, n_y = lax.axis_size("gz"), lax.axis_size("gy")
    nz, ny, nx = estimate.shape
    fits = n_y == 2 and n_z % 4 == 0 and nx == 4 * LANES and nz == 16 and 2 * ny == 64
    if fits:
        return slabs(n_z // 2, estimate, measured, psf_z, psf_y, psf_x, extents, order)
    return general(estimate, measured, psf_z, psf_y, psf_x, extents, order)


def solution(mesh):
    return jax.shard_map(
        on_device,
        mesh=mesh,
        in_specs=(P("gz", "gy", None), P(None, "gz", "gy", None), P(), P(), P(), P(), P()),
        out_specs=P("gz", "gy", None),
        check_vma=False,
    )
```
